256 devices in a mesh: layer: 4 (over y), rep: 2 (over core), row: 4 (over x), col: 8 (over z).
Axes of the slice: x: 4, y: 4, z: 8, core: 2. Of those that a mesh axis runs over, the one named last changes fastest.
Arguments:
- iterate: bfloat16 [14336, 8192], P(('layer', 'row'), ('rep', 'col')), parts along dimension 0, may hold values from -0.03125 to 0.03125
Outputs:
- next_iterate: bfloat16 [14336, 8192], P(('layer', 'row'), ('rep', 'col')), parts along dimension 0
The draws below stay inside these ranges and needn't reach their ends.
There are 4 independent parts, one for each index of `layer`. The reference program is written for one: setup_inputs(seed, part) draws one part's arguments, and reference() takes and returns one part's arrays. A program takes and returns all parts, laid end to end along the dimension named above; each array names one. Nothing has to cross between parts.
All inputs are finite; a program needn't handle non-finite values.
Results may differ from the reference program's by a relative error of at most 0.017.
Values may be sent and summed in bfloat16 or wider, within the bound.
A program may use at most 64 MiB of HBM per device.

```python
import jax
import jax.numpy as jnp
from jax import lax

COLS = 8192
ROWS = 3584
BLOCKS = 16


def levels(stream_key, dims, shards, least, top_value):
    factor_of = 1.0
    for position, parts in shards:
        heights = jax.random.uniform(jax.random.fold_in(jax.random.fold_in(stream_key, 6), position), (parts,), jnp.float32, least / len(shards), top_value / len(shards))
        factor_of = factor_of * jnp.repeat(jnp.exp(heights), dims[position] // parts).reshape((-1,) + (1,) * (len(dims) - 1 - position))
    return factor_of


def noise(stream_key, extent, deviation, most, cuts=(), kind=jnp.bfloat16):
    gain = levels(stream_key, extent, cuts, -0.22, 0.18) if cuts else 1.0
    array = jax.random.normal(stream_key, extent, jnp.float32) * deviation * gain
    return jnp.minimum(jnp.maximum(array, -most), most).astype(kind)


def setup_inputs(seed: int = 0, part: int = 0) -> dict:
    key_of = jax.random.split(jax.random.key(seed), 2)
    part_splits = jax.random.split(jax.random.fold_in(key_of[1], part), 2)
    iterate = noise(part_splits[0], (ROWS, COLS), (4 * COLS) ** -0.5, 0.03125, ((0, 4), (1, 16)))
    return {"iterate": iterate}


coef_linear = 3.4445
coef_cubic = -4.775
coef_quintic = 2.0315

def reference(iterate):
    block_width = COLS // BLOCKS
    col_blocks = iterate.reshape(ROWS, BLOCKS, block_width).transpose(1, 0, 2)

    def add_gram(running, x_block):
        partial_sum = jnp.dot(x_block, x_block.T, preferred_element_type=jnp.float32).astype(jnp.bfloat16)
        partial_sum = lax.optimization_barrier(partial_sum)
        return (running + partial_sum.astype(jnp.float32), None)
    gram_sum, _ = lax.scan(add_gram, jnp.zeros((ROWS, ROWS), jnp.float32), col_blocks)
    gram_sum = gram_sum.astype(jnp.bfloat16)
    square_width = ROWS // BLOCKS
    left_blocks = gram_sum.reshape(ROWS, BLOCKS, square_width).transpose(1, 0, 2)
    right_blocks = gram_sum.reshape(BLOCKS, square_width, ROWS)

    def add_square(running, pair_blocks):
        partial_sum = jnp.dot(pair_blocks[0], pair_blocks[1], preferred_element_type=jnp.float32).astype(jnp.bfloat16)
        partial_sum = lax.optimization_barrier(partial_sum)
        return (running + partial_sum.astype(jnp.float32), None)
    square, _ = lax.scan(add_square, jnp.zeros((ROWS, ROWS), jnp.float32), (left_blocks, right_blocks))
    combo = (coef_cubic * gram_sum.astype(jnp.float32) + coef_quintic * square).astype(jnp.bfloat16)
    product = jnp.dot(combo, iterate, preferred_element_type=jnp.float32)
    scale_factor = 0.2 * jnp.sqrt(jnp.float32(COLS))
    return (scale_factor * (coef_linear * iterate.astype(jnp.float32) + product)).astype(jnp.bfloat16)
```

```python
import functools

import jax
import jax.numpy as jnp
from jax import lax
from jax.experimental import pallas as pl
from jax.experimental.pallas import tpu as pltpu
from jax.sharding import PartitionSpec as P

COLS = 8192

coef_linear = 3.4445
coef_cubic = -4.775
coef_quintic = 2.0315
MESH = pl.DeviceIdType.MESH
f32 = jnp.float32
bf16 = jnp.bfloat16


def dot(left, right):
    return jnp.dot(left, right, preferred_element_type=f32)


def dot_t(left, right):
    return lax.dot_general(
        left, right, (((1,), (1,)), ((), ())), preferred_element_type=f32
    )


def kernel(nz, sizes, x_ref, o_ref, xo, xq, g, part, rl, rs, v, acc, ob, ssem, rsem, lsem):
    core = lax.axis_index("rep")
    r = lax.axis_index("row")
    z = lax.axis_index("col")
    rows, width = x_ref.shape
    strip = rows // nz
    far, near = nz // 2, nz // 2 - 1
    units = range(len(sizes))
    offs = [sum(sizes[:u]) for u in units]
    right = {"row": lax.rem(r + 1, 4)}
    left = {"row": lax.rem(r + 3, 4)}
    partner = {"rep": 1 - core}
    keys = {}

    def at_z(k):
        return lax.rem(z + (k % nz), nz)

    def chunk(u):
        return pl.ds(nz * offs[u], nz * sizes[u])

    def piece(u, d):
        return pl.ds(pl.multiple_of(nz * offs[u] + d * sizes[u], 16), sizes[u])

    def slot(u):
        return pl.ds(offs[u], sizes[u])

    def way(t, u):
        return 1 if (t + u) % 2 == 0 else -1

    def rel(t, c=core):
        return 3 * c if t == 0 else 2 - c

    def link(key, src, dst, dev):
        i = keys.setdefault(key, len(keys))
        return pltpu.make_async_remote_copy(
            src_ref=src, dst_ref=dst, send_sem=ssem.at[i], recv_sem=rsem.at[i],
            device_id=dev, device_id_type=MESH,
        )

    def hop(buf, key, d, u):
        return link(
            key, buf.at[0, chunk(u)], buf.at[3 if d > 0 else 1, chunk(u)],
            right if d > 0 else left,
        )

    def relay(buf, key, d, u):
        return link(
            key, buf.at[3 if d > 0 else 1, chunk(u)], buf.at[2, chunk(u)],
            right if d > 0 else left,
        )

    def desc(key, incoming=False):
        kind = key[0]
        if kind == "X":
            return hop(xo, key, key[1], key[2])
        if kind == "V":
            return hop(v, key, key[1], key[2])
        if kind == "F":
            return relay(xo, key, key[1], key[2])
        if kind == "W":
            return relay(v, key, key[1], key[2])
        if kind == "P":
            _, k, u = key
            return link(key, xo.at[k, chunk(u)], xq.at[k, chunk(u)], partner)
        if kind == "G":
            _, t, u = key
            k = rel(t, 1 - core) if incoming else rel(t)
            return link(key, g.at[k, chunk(u)], g.at[k, chunk(u)], partner)
        _, t, u, s = key
        w = way(t, u)
        if kind == "RL":
            src = part.at[t, piece(u, at_z(far * w))] if s == 0 else rl.at[t, s - 1, slot(u)]
            return link(key, src, rl.at[t, s, slot(u)], {"col": at_z(w)})
        if kind == "RS":
            src = part.at[t, piece(u, at_z(-near * w))] if s == 0 else rs.at[t, s - 1, slot(u)]
            return link(key, src, rs.at[t, s, slot(u)], {"col": at_z(-w)})
        step = s + 1 if incoming else s
        if kind == "AL":
            here = g.at[rel(t), piece(u, at_z(-step * w))]
            return link(key, here, here, {"col": at_z(w)})
        here = g.at[rel(t), piece(u, at_z(step * w))]
        return link(key, here, here, {"col": at_z(-w)})

    sent = []

    def send(*key):
        desc(key).start()
        sent.append(key)

    def take(*key):
        desc(key, True).wait_recv()

    def gram(t, u):
        k = rel(t)
        mine, his = xo[0, chunk(u)], xq[0, chunk(u)]

        def columns(at, n):
            there = pl.ds(at, n)
            part[t, chunk(u), there] = (
                dot_t(mine, xo[k, there]) + dot_t(his, xq[k, there])
            ).astype(bf16)

        wide = rows // 256

        @pl.loop(0, wide)
        def _(i):
            columns(pl.multiple_of(i * 256, 256), 256)

        if rows % 256:
            columns(wide * 256, rows % 256)

    def begin(t, u):
        gram(t, u)
        send("RL", t, u, 0)
        send("RS", t, u, 0)

    def plus(buf, t, u, s, d):
        buf[t, s, slot(u)] = (
            buf[t, s, slot(u)].astype(f32) + part[t, piece(u, d)].astype(f32)
        ).astype(bf16)

    def reduce_step(t, u, s):
        w = way(t, u)
        take("RL", t, u, s)
        if s < far - 1:
            plus(rl, t, u, s, at_z((far - 1 - s) * w))
            send("RL", t, u, s + 1)
        if s < near:
            take("RS", t, u, s)
            if s < near - 1:
                plus(rs, t, u, s, at_z(-(near - 1 - s) * w))
                send("RS", t, u, s + 1)
        if s == far - 1:
            g[rel(t), piece(u, z)] = (
                rl[t, far - 1, slot(u)].astype(f32)
                + rs[t, near - 1, slot(u)].astype(f32)
                + part[t, piece(u, z)].astype(f32)
            ).astype(bf16)
            send("AL", t, u, 0)
            send("AS", t, u, 0)

    def gather_step(t, u, s):
        take("AL", t, u, s)
        if s < far - 1:
            send("AL", t, u, s + 1)
        if s < near:
            take("AS", t, u, s)
            if s < near - 1:
                send("AS", t, u, s + 1)
        if s == far - 1:
            send("G", t, u)

    loads = [
        pltpu.make_async_copy(
            x_ref.at[pl.ds(d * strip + offs[u], sizes[u])],
            xo.at[0, pl.ds(nz * offs[u] + d * sizes[u], sizes[u])],
            lsem.at[u * nz + d],
        )
        for u in units
        for d in range(nz)
    ]
    for load in loads:
        load.start()
    barrier = pltpu.get_barrier_semaphore()
    for dev in (right, left, partner, {"col": at_z(1)}, {"col": at_z(-1)}):
        pl.semaphore_signal(barrier, inc=1, device_id=dev, device_id_type=MESH)
    pl.semaphore_wait(barrier, 5)
    for load in loads:
        load.wait()

    send("P", 0, 0)
    send("P", 0, 1)
    send("X", 1, 0)
    send("X", -1, 1)
    send("X", 1, 1)
    send("X", -1, 0)
    take("P", 0, 0)
    take("P", 0, 1)
    common = list(sent)

    def pass_on(share):
        take("X", 1, 0)
        send("F", 1, 0)
        take("X", -1, 1)
        send("F", -1, 1)
        if share:
            send("P", 3, 0)
            send("P", 1, 1)

    def rest_of_ones(share):
        take("X", 1, 1)
        take("X", -1, 0)
        if share:
            send("P", 3, 1)
            send("P", 1, 0)

    def twos(share):
        take("F", 1, 0)
        take("F", -1, 1)
        if share:
            send("P", 2, 0)
            send("P", 2, 1)

    sent.clear()

    @pl.when(core == 0)
    def _():
        for u in units:
            begin(0, u)
        for s in range(far):
            for u in units:
                reduce_step(0, u, s)
        pass_on(True)
        for s in range(far):
            for u in units:
                gather_step(0, u, s)
        rest_of_ones(True)
        twos(False)
        take("P", 2, 0)
        take("P", 2, 1)
        for u in units:
            begin(1, u)
        for s in range(far):
            for u in units:
                reduce_step(1, u, s)
        for s in range(far):
            for u in units:
                gather_step(1, u, s)

    zero_sent = list(sent)
    sent.clear()

    @pl.when(core == 1)
    def _():
        pass_on(False)
        rest_of_ones(False)
        for k in (3, 1):
            for u in units:
                take("P", k, u)
        for u in units:
            for t in (0, 1):
                begin(t, u)
        for s in range(far):
            if s == far // 2:
                twos(True)
            for u in units:
                for t in (0, 1):
                    reduce_step(t, u, s)
        for s in range(far):
            for u in units:
                for t in (0, 1):
                    gather_step(t, u, s)

    one_sent = list(sent)
    sent.clear()

    for u in units:
        take("G", 0, u)
        take("G", 1, u)
        here = acc.at[pl.ds(0, nz * sizes[u])]
        here[...] = coef_cubic * xo[0, chunk(u)].astype(f32)

        @pl.loop(0, 4)
        def _(k):
            here[...] += coef_quintic * dot(g[k, chunk(u)], xo[k])

        v[0, chunk(u)] = here[...].astype(bf16)
        send("V", 1, u)
        send("V", -1, u)

    half = rows // 2

    def apply(k):
        @pl.loop(0, 2)
        def _(i):
            part_rows = pl.ds(pl.multiple_of(i * half, half), half)
            acc[part_rows] += dot(g[k, part_rows], v[k])

    acc[...] = coef_linear * xo[0].astype(f32)
    apply(0)
    take("V", 1, 0)
    send("W", 1, 0)
    take("V", -1, 0)
    take("V", -1, 1)
    send("W", -1, 1)
    take("V", 1, 1)
    apply(3)
    apply(1)
    take("W", 1, 0)
    take("W", -1, 1)
    apply(2)
    scale = 0.2 * jnp.sqrt(f32(COLS))
    ob[...] = (scale * acc[...]).astype(bf16)
    stores = [
        pltpu.make_async_copy(
            ob.at[pl.ds(nz * offs[u] + d * sizes[u], sizes[u])],
            o_ref.at[pl.ds(d * strip + offs[u], sizes[u])],
            lsem.at[u * nz + d],
        )
        for u in units
        for d in range(nz)
    ]
    for store in stores:
        store.start()

    def drain(some):
        for key in some:
            desc(key).wait_send()

    drain(common + sent)

    @pl.when(core == 0)
    def _():
        drain(zero_sent)

    @pl.when(core == 1)
    def _():
        drain(one_sent)

    for store in stores:
        store.wait()


def local(nz, iterate):
    rows, width = iterate.shape
    strip = rows // nz
    first = -(-strip // 32) * 16
    sizes = (first, strip - first)
    far = nz // 2
    return pl.pallas_call(
        functools.partial(kernel, nz, sizes),
        out_shape=jax.ShapeDtypeStruct((rows, width), bf16),
        in_specs=[pl.BlockSpec(memory_space=pl.ANY)],
        out_specs=pl.BlockSpec(memory_space=pl.ANY),
        scratch_shapes=[
            pltpu.VMEM((4, rows, width), bf16),
            pltpu.VMEM((4, rows, width), bf16),
            pltpu.VMEM((4, rows, rows), bf16),
            pltpu.VMEM((2, rows, rows), bf16),
            pltpu.VMEM((2, far, strip, rows), bf16),
            pltpu.VMEM((2, far - 1, strip, rows), bf16),
            pltpu.VMEM((4, rows, width), bf16),
            pltpu.VMEM((rows, width), f32),
            pltpu.VMEM((rows, width), bf16),
            pltpu.SemaphoreType.DMA((96,)),
            pltpu.SemaphoreType.DMA((96,)),
            pltpu.SemaphoreType.DMA((2 * nz,)),
        ],
        compiler_params=pltpu.CompilerParams(
            collective_id=0, has_side_effects=True, vmem_limit_bytes=60 * 1024 * 1024
        ),
    )(iterate)


def solution(mesh):
    spec = P(("layer", "row"), ("rep", "col"))
    step = functools.partial(local, mesh.shape["col"])
    return jax.shard_map(step, mesh=mesh, in_specs=(spec,), out_specs=spec, check_vma=False)
```
